32 devices in a mesh: grp: 1, sp: 32 (over z, y, x, core), ch: 1.
Axes of the slice: x: 2, y: 2, z: 4, core: 2. Of those that a mesh axis runs over, the one named last changes fastest.
Arguments:
- latents: bfloat16 [131072, 1024], P(('grp', 'sp')), may hold values from -6 to 6
- spectrum: bfloat16 [16, 64, 128, 1024], P(None, None, 'sp', 'ch'), may hold values from -4 to 4
- w_value: bfloat16 [1024, 1024], P('sp', 'ch'), may hold values from -0.1875 to 0.1875
- w_gate: bfloat16 [1024, 1024], P('sp', 'ch'), may hold values from -0.1875 to 0.1875
- w_out: bfloat16 [1024, 1024], P('sp'), may hold values from -0.1875 to 0.1875
- embed_table: bfloat16 [1024, 32768], P(('sp', 'ch')), may hold values from -12 to 12
- prompt_ids: int32 [256], P('grp'), may hold values from 0 to 32767
- noise_step: int32 [1], P('grp'), may hold values from 0 to 999
Outputs:
- denoised: bfloat16 [131072, 1024], P(('grp', 'sp', 'ch'))
The draws below stay inside these ranges and needn't reach their ends.
All inputs are finite; a program needn't handle non-finite values.
Results may differ from the reference program's by a relative error of at most 0.013.
Values may be sent and summed in bfloat16 or wider, within the bound.
No kernel may reach another device: no remote copies, remote signals or barrier semaphores. Data moves between devices by JAX's collectives and lax.ppermute only.
A program may use at most 128 MiB of HBM per device.

```python
import math
import jax
import jax.numpy as jnp
import numpy as np
from jax import lax

TT = 16
HH = 64
WW = 128
C = 1024
VOCAB = 32768
PROMPT = 256
CELLS = 131072


def plant(drawn, own_key, low, high):
    longest = drawn.shape.index(max(drawn.shape))
    spots = []
    for shift in (0, 1):
        where = [jax.random.randint(jax.random.fold_in(own_key, axis), (), 0, length) for axis, length in enumerate(drawn.shape)]
        where[longest] = (where[longest] + shift) % drawn.shape[longest]
        spots.append(tuple(where))
    return drawn.at[spots[0]].set(low).at[spots[1]].set(high)


def shard_levels(key, dims, cuts, least, top_value):
    loudness, own = 1.0, jax.random.fold_in(key, 6)
    for axis_at, shards_of in cuts:
        draws = jnp.exp(jax.random.uniform(jax.random.fold_in(own, axis_at), (shards_of,), jnp.float32, least / len(cuts), top_value / len(cuts)))
        loudness = loudness * jnp.repeat(draws, dims[axis_at] // shards_of).reshape([-1 if axis == axis_at else 1 for axis in range(len(dims))])
    return loudness


def rank_table(amount, slope):
    weights = [(1 << 20) // math.isqrt(grade ** slope) + 1 for grade in range(1, amount + 1)]
    width = 1 + sum(weights) // (1 << 30)
    return np.cumsum(np.array([max(1, weight // width) for weight in weights]))


def ranked(key, dims, count, lean):
    table = rank_table(count, lean)
    lot = jax.random.randint(jax.random.fold_in(key, 1), dims, 0, int(table[count - 1]))
    rank = jnp.searchsorted(jnp.asarray(table, jnp.int32), lot, side="right")
    return jax.random.permutation(jax.random.fold_in(key, 2), count)[rank].astype(jnp.int32)


def bell_draw(own_key, dims, scale, limit, cuts=(), held_as=jnp.bfloat16):
    values = scale * jax.random.normal(own_key, dims, jnp.float32)
    if cuts:
        values = values * shard_levels(own_key, dims, cuts, -0.22, 0.18)
    return jnp.clip(values, -limit, limit).astype(held_as)


def setup_inputs(seed: int = 0, part: int = 0) -> dict:
    key_list = jax.random.split(jax.random.key(seed), 9)
    part_keys = jax.random.split(jax.random.fold_in(key_list[8], part), 9)
    latents = bell_draw(part_keys[0], (CELLS, C), 1.0, 6.0, ((0, 32),))
    spectrum = bell_draw(key_list[1], (TT, HH, WW, C), 1.0, 4.0, ((2, 32),))
    w_value = bell_draw(key_list[2], (C, C), C ** -0.5, 0.1875, ((0, 32),))
    w_gate = bell_draw(key_list[3], (C, C), C ** -0.5, 0.1875, ((0, 32),))
    w_out = bell_draw(key_list[4], (C, C), C ** -0.5, 0.1875, ((0, 32),))
    embed_table = bell_draw(key_list[5], (C, VOCAB), 3.0, 12.0, ((0, 32),))
    prompt_ids = plant(ranked(part_keys[6], (PROMPT,), VOCAB, 2), jax.random.fold_in(part_keys[6], 3), 0, VOCAB - 1).astype(jnp.int32)
    noise_step = jax.random.randint(part_keys[7], (1,), 0, 1000).astype(jnp.int32)
    return {"latents": latents, "spectrum": spectrum, "w_value": w_value, "w_gate": w_gate, "w_out": w_out, "embed_table": embed_table, "prompt_ids": prompt_ids, "noise_step": noise_step}


def cas_table(length):
    position = jnp.arange(length, dtype=jnp.int32)
    product = position[:, None] * position[None, :] % length
    phase_angle = product.astype(jnp.float32) * (2.0 * math.pi / length)
    return ((jnp.cos(phase_angle) + jnp.sin(phase_angle)) / math.sqrt(length)).astype(jnp.bfloat16)

def step_embedding(noise_step, channel, channels):
    half_count = channels // 2
    lower_half = channel < half_count
    position = jnp.where(lower_half, channel, channel - half_count).astype(jnp.float32)
    frequency = jnp.exp(-math.log(10000.0) * position / half_count)
    phase_angle = noise_step[0].astype(jnp.float32) * frequency
    return jnp.where(lower_half, jnp.sin(phase_angle), jnp.cos(phase_angle))

def apply_table(form, table, operand):
    return jnp.einsum(form, table.astype(jnp.float32), operand.astype(jnp.float32), precision=lax.Precision.HIGHEST)

def reference(latents, spectrum, w_value, w_gate, w_out, embed_table, prompt_ids, noise_step):
    channel = jnp.arange(C, dtype=jnp.int32)
    pooled = lax.optimization_barrier(jnp.mean(jnp.take(embed_table, prompt_ids, axis=1).astype(jnp.float32), axis=1))
    modulation = 1.0 + pooled + step_embedding(noise_step, channel, C)
    value_rows = jnp.dot(latents, w_value, preferred_element_type=jnp.float32).astype(jnp.bfloat16)
    gate_rows = jnp.dot(latents, w_gate, preferred_element_type=jnp.float32)
    cas_width = cas_table(WW)
    cas_height = cas_table(HH)
    cas_time = cas_table(TT)
    latent_grid = value_rows.reshape(TT, HH, WW, C)
    width_spec = apply_table('kw,thwc->thkc', cas_width, latent_grid).astype(jnp.bfloat16)
    height_spec = apply_table('ah,thkc->takc', cas_height, width_spec).astype(jnp.bfloat16)
    full_spec = apply_table('st,takc->sakc', cas_time, height_spec).astype(jnp.bfloat16)
    filtered = (full_spec.astype(jnp.float32) * spectrum.astype(jnp.float32)).astype(jnp.bfloat16)
    time_back = apply_table('ts,sakc->takc', cas_time, filtered).astype(jnp.bfloat16)
    height_back = apply_table('ha,takc->thkc', cas_height, time_back).astype(jnp.bfloat16)
    mix_rows = apply_table('wk,thkc->thwc', cas_width, height_back).reshape(TT * HH * WW, C)
    mixed_rows = (mix_rows * jax.nn.silu(gate_rows) * modulation[None, :]).astype(jnp.bfloat16)
    projected = jnp.dot(mixed_rows, w_out, preferred_element_type=jnp.float32)
    return (latents.astype(jnp.float32) + projected).astype(jnp.bfloat16)
```

```python
import functools
import math

import jax
import jax.numpy as jnp
import numpy as np
from jax import lax
from jax.experimental import pallas as pl
from jax.experimental.pallas import tpu as pltpu
from jax.sharding import PartitionSpec as P

TT = 16
HH = 64
WW = 128
C = 1024


def cas_table(length):
    position = jnp.arange(length, dtype=jnp.int32)
    product = position[:, None] * position[None, :] % length
    phase_angle = product.astype(jnp.float32) * (2.0 * math.pi / length)
    return ((jnp.cos(phase_angle) + jnp.sin(phase_angle)) / math.sqrt(length)).astype(jnp.bfloat16)


def step_embedding(noise_step, channel, channels):
    half_count = channels // 2
    lower_half = channel < half_count
    position = jnp.where(lower_half, channel, channel - half_count).astype(jnp.float32)
    frequency = jnp.exp(-math.log(10000.0) * position / half_count)
    phase_angle = noise_step[0].astype(jnp.float32) * frequency
    return jnp.where(lower_half, jnp.sin(phase_angle), jnp.cos(phase_angle))


def apply_table(form, table, operand):
    return jnp.einsum(form, table, operand, preferred_element_type=jnp.float32)


def local_split_channels(latents, spectrum, w_value, w_gate, w_out, embed_table, prompt_ids, noise_step):
    row_count = latents.shape[0]
    chan_part = w_value.shape[1]
    full_value, full_gate, full_out = (
        lax.all_gather(w_value, "sp", axis=0, tiled=True),
        lax.all_gather(w_gate, "sp", axis=0, tiled=True),
        lax.all_gather(w_out, "sp", axis=0, tiled=True),
    )
    value_rows = jnp.dot(latents, full_value, preferred_element_type=jnp.float32).astype(
        jnp.bfloat16
    )
    gate_rows = jnp.dot(latents, full_gate, preferred_element_type=jnp.float32)
    cas_width = cas_table(WW)
    cas_height = cas_table(HH)
    cas_time = cas_table(TT)
    line_grid = value_rows.reshape(row_count // WW, WW, chan_part)
    width_spec = apply_table("kw,lwc->lkc", cas_width, line_grid).astype(jnp.bfloat16)
    pencil = lax.all_to_all(width_spec, "sp", split_axis=1, concat_axis=0, tiled=True)
    band_count = pencil.shape[1]
    pencil = pencil.reshape(TT, HH, band_count, chan_part)
    height_spec = apply_table("ah,thkc->takc", cas_height, pencil).astype(jnp.bfloat16)
    full_spec = apply_table("st,takc->sakc", cas_time, height_spec).astype(jnp.bfloat16)
    filtered = (full_spec.astype(jnp.float32) * spectrum.astype(jnp.float32)).astype(jnp.bfloat16)
    time_back = apply_table("ts,sakc->takc", cas_time, filtered).astype(jnp.bfloat16)
    height_back = apply_table("ha,takc->thkc", cas_height, time_back).astype(jnp.bfloat16)
    returned = lax.all_to_all(
        height_back.reshape(TT * HH, band_count, chan_part),
        "sp",
        split_axis=0,
        concat_axis=1,
        tiled=True,
    )
    mix_rows = apply_table("wk,lkc->lwc", cas_width, returned).reshape(row_count, chan_part)
    offset = lax.axis_index("ch") * chan_part
    local_pool = jnp.mean(jnp.take(embed_table, prompt_ids, axis=1).astype(jnp.float32), axis=1)
    pooled_all = lax.all_gather(local_pool, ("sp", "ch"), axis=0, tiled=True)
    pooled = lax.dynamic_slice_in_dim(pooled_all, offset, chan_part)
    channel = offset + jnp.arange(chan_part, dtype=jnp.int32)
    modulation = 1.0 + pooled + step_embedding(noise_step, channel, C)
    mixed_rows = (mix_rows * jax.nn.silu(gate_rows) * modulation[None, :]).astype(jnp.bfloat16)
    half_rows = row_count // lax.axis_size("ch")
    own_rows = lax.dynamic_slice_in_dim(full_out, offset, chan_part, 0)
    summed = lax.psum_scatter(
        jnp.dot(mixed_rows, own_rows, preferred_element_type=jnp.float32).astype(jnp.bfloat16),
        "ch",
        scatter_dimension=0,
        tiled=True,
    ).astype(jnp.float32)
    residual = lax.dynamic_slice_in_dim(latents, lax.axis_index("ch") * half_rows, half_rows, 0)
    return (residual.astype(jnp.float32) + summed).astype(jnp.bfloat16)

SUB = 8
MIB = 1 << 20


def cas_host(length):
    position = np.arange(length)
    phase_angle = (position[:, None] * position[None, :] % length).astype(np.float32) * np.float32(
        2.0 * math.pi / length
    )
    table = (np.cos(phase_angle) + np.sin(phase_angle)) / np.float32(math.sqrt(length))
    return table.astype(jnp.bfloat16).astype(np.float32)


def width_table(devices, band_count, bands):
    frequency = (np.arange(devices)[:, None] * band_count + np.asarray(bands)[None, :]).reshape(-1)
    rows = cas_host(WW)[frequency]
    return np.einsum("fw,lm->flmw", rows, np.eye(SUB, dtype=np.float32)).reshape(
        len(frequency) * SUB, SUB * WW
    ).astype(jnp.bfloat16)


def plane_table():
    return np.kron(cas_host(TT), cas_host(HH)).astype(jnp.bfloat16)


def dot32(left, right, contract=(1, 0)):
    return lax.dot_general(
        left, right, (((contract[0],), (contract[1],)), ((), ())), preferred_element_type=jnp.float32
    )


def forward_body(table_ref, rows_ref, out_ref):
    spec = dot32(table_ref[...], rows_ref[...])
    out_ref[...] = spec.reshape(out_ref.shape).astype(jnp.bfloat16)


def width_forward(table, latents, devices, bands):
    rows, chans = latents.shape
    group = SUB * WW
    lines = rows // WW
    return pl.pallas_call(
        forward_body,
        name="width_forward",
        grid=(rows // group,),
        in_specs=[
            pl.BlockSpec(table.shape, lambda g: (0, 0)),
            pl.BlockSpec((group, chans), lambda g: (g, 0)),
        ],
        out_specs=pl.BlockSpec((devices, bands, SUB, chans), lambda g: (0, 0, g, 0)),
        out_shape=jax.ShapeDtypeStruct((devices, bands, lines, chans), jnp.bfloat16),
        compiler_params=pltpu.CompilerParams(
            dimension_semantics=("arbitrary",), vmem_limit_bytes=58 * MIB
        ),
        cost_estimate=pl.CostEstimate(
            flops=2 * rows * chans * table.shape[0],
            bytes_accessed=4 * rows * chans,
            transcendentals=0,
        ),
    )(table, latents)


def plane_body(table_ref, value_ref, spectrum_ref, pencil_ref, out_ref, first_ref, second_ref):
    cells, chans = first_ref.shape
    step = min(cells, 256)
    pencil = pencil_ref[...].reshape(cells, chans)
    for at in range(0, cells, step):
        part = pl.ds(at, step)
        first_ref[part, :] = dot32(table_ref[part, :], pencil).astype(jnp.bfloat16)
    for at in range(0, cells, step):
        part = pl.ds(at, step)
        full = dot32(first_ref[part, :], value_ref[...])
        gain = spectrum_ref[0, part, :].astype(jnp.float32)
        second_ref[part, :] = (full * gain).astype(jnp.bfloat16)
    devices, _, lines, _ = out_ref.shape
    per = step // lines
    for at in range(0, cells, step):
        back = dot32(table_ref[pl.ds(at, step), :], second_ref[...]).astype(jnp.bfloat16)
        out_ref[pl.ds(at // lines, per), :, :, :] = back.reshape(per, 1, lines, chans)


def plane_filter(table, w_value, spectrum, pencil, first_band):
    devices, bands, lines, chans = pencil.shape
    cells = devices * lines
    block = pl.BlockSpec((devices, 1, lines, chans), lambda j: (0, j, 0, 0))
    return pl.pallas_call(
        plane_body,
        name="plane_filter",
        grid=(bands,),
        in_specs=[
            pl.BlockSpec(table.shape, lambda j: (0, 0)),
            pl.BlockSpec(w_value.shape, lambda j: (0, 0)),
            pl.BlockSpec((1, cells, chans), lambda j: (first_band + j, 0, 0)),
            block,
        ],
        out_specs=block,
        out_shape=jax.ShapeDtypeStruct(pencil.shape, jnp.bfloat16),
        scratch_shapes=[pltpu.VMEM((cells, chans), jnp.bfloat16)] * 2,
        compiler_params=pltpu.CompilerParams(
            dimension_semantics=("arbitrary",), vmem_limit_bytes=58 * MIB
        ),
        cost_estimate=pl.CostEstimate(
            flops=2 * bands * cells * chans * (2 * cells + chans),
            bytes_accessed=6 * bands * cells * chans,
            transcendentals=0,
        ),
    )(table, w_value, spectrum, pencil)


def finish_body(*refs):
    parts = (len(refs) - 4) // 2
    tables, spectra = refs[:parts], refs[parts : 2 * parts]
    gate_ref, latents_ref, w_out_ref, out_ref = refs[2 * parts :]
    chans = out_ref.shape[1]
    mix = None
    for table_ref, spec_ref in zip(tables, spectra):
        spec = spec_ref[...].astype(jnp.float32).reshape(table_ref.shape[0], chans)
        term = dot32(table_ref[...], spec.astype(jnp.bfloat16), (0, 0))
        mix = term if mix is None else mix + term
    mixed = (mix * gate_ref[...].astype(jnp.float32)).astype(jnp.bfloat16)
    out = latents_ref[...].astype(jnp.float32) + dot32(mixed, w_out_ref[...])
    out_ref[...] = out.astype(jnp.bfloat16)


def finish(tables, spectra, gate, latents, w_out):
    rows, chans = latents.shape
    group = SUB * WW
    by_group = pl.BlockSpec((group, chans), lambda g: (g, 0))
    whole = lambda g: (0, 0)
    return pl.pallas_call(
        finish_body,
        name="finish",
        grid=(rows // group,),
        in_specs=[pl.BlockSpec(table.shape, whole) for table in tables]
        + [
            pl.BlockSpec(spec.shape[:2] + (SUB, chans), lambda g: (0, 0, g, 0))
            for spec in spectra
        ]
        + [by_group, by_group, pl.BlockSpec(w_out.shape, whole)],
        out_specs=by_group,
        out_shape=jax.ShapeDtypeStruct((rows, chans), jnp.bfloat16),
        compiler_params=pltpu.CompilerParams(
            dimension_semantics=("arbitrary",), vmem_limit_bytes=58 * MIB
        ),
        cost_estimate=pl.CostEstimate(
            flops=2 * rows * chans * (group + chans),
            bytes_accessed=8 * rows * chans,
            transcendentals=0,
        ),
    )(*tables, *spectra, gate, latents, w_out)


def gather_blocks(block, axis, devices):
    own = lax.axis_index(axis)
    held = block[None]
    bit = devices // 2
    order = []
    while bit:
        pairs = [(i, i ^ bit) for i in range(devices)]
        other = lax.ppermute(held, axis, pairs)
        held = jnp.concatenate([held, other], axis=0)
        order = order + [slot ^ bit for slot in order] if order else [0, bit]
        bit //= 2
    slot_of = np.argsort(np.asarray(order))
    return held, slot_of, own


def in_device_order(held, slot_of, own):
    devices = held.shape[0]
    slots = jnp.asarray(slot_of, jnp.int32)[jnp.arange(devices, dtype=jnp.int32) ^ own]
    return jnp.take(held, slots, axis=0)


def local_planes(
    devices, latents, spectrum, w_value, w_gate, w_out, embed_table, prompt_ids, noise_step
):
    row_count, chans = latents.shape
    band_count = spectrum.shape[2]
    half = max(band_count // 2, 1)
    chunks = [tuple(range(at, min(at + half, band_count))) for at in range(0, band_count, half)]
    tables = [jnp.asarray(width_table(devices, band_count, bands)) for bands in chunks]
    plane = jnp.asarray(plane_table())

    sent = [width_forward(table, latents, devices, len(b)) for table, b in zip(tables, chunks)]
    pencils = [
        lax.all_to_all(part, "sp", split_axis=0, concat_axis=0, tiled=True) for part in sent
    ]

    weights = jnp.concatenate([w_value, w_gate, w_out], axis=0)
    held, slot_of, own = gather_blocks(weights, "sp", devices)
    ordered = in_device_order(held, slot_of, own)
    per = w_value.shape[0]
    full_value = ordered[:, :per].reshape(-1, chans)
    full_gate = ordered[:, per : 2 * per].reshape(-1, chans)
    full_out = ordered[:, 2 * per :].reshape(-1, chans)

    local_pool = jnp.mean(jnp.take(embed_table, prompt_ids, axis=1).astype(jnp.float32), axis=1)
    pool_held, pool_slot, _ = gather_blocks(local_pool, "sp", devices)
    pooled = in_device_order(pool_held, pool_slot, own).reshape(-1)
    channel = jnp.arange(chans, dtype=jnp.int32)
    modulation = 1.0 + pooled + step_embedding(noise_step, channel, chans)
    gate_rows = jnp.dot(latents, full_gate, preferred_element_type=jnp.float32)
    gate = (jax.nn.silu(gate_rows) * modulation[None, :]).astype(jnp.bfloat16)

    gain = spectrum.transpose(2, 0, 1, 3).reshape(band_count, TT * HH, chans)
    returned = [
        lax.all_to_all(
            plane_filter(plane, full_value, gain, pencil, bands[0]),
            "sp",
            split_axis=0,
            concat_axis=0,
            tiled=True,
        )
        for pencil, bands in zip(pencils, chunks)
    ]
    return finish(tables, returned, gate, latents, full_out)


def solution(mesh):
    placed = (
        P(("grp", "sp"), None),
        P(None, None, "sp", "ch"),
        P("sp", "ch"),
        P("sp", "ch"),
        P("sp", None),
        P(("sp", "ch"), None),
        P("grp"),
        P("grp"),
    )
    devices = mesh.shape["sp"]
    lines = TT * HH // devices
    planes = mesh.shape["ch"] == 1 and devices & (devices - 1) == 0 and lines % SUB == 0
    local = functools.partial(local_planes, devices) if planes else local_split_channels
    return jax.shard_map(
        local, mesh=mesh, in_specs=placed, out_specs=P(("grp", "sp", "ch"), None), check_vma=False
    )
```

```python
import functools
import math

import jax
import jax.numpy as jnp
import numpy as np
from jax import lax
from jax.experimental import pallas as pl
from jax.experimental.pallas import tpu as pltpu
from jax.sharding import PartitionSpec as P


TT = 16
HH = 64
WW = 128
C = 1024


def cas_table(length):
    position = jnp.arange(length, dtype=jnp.int32)
    product = position[:, None] * position[None, :] % length
    phase_angle = product.astype(jnp.float32) * (2.0 * math.pi / length)
    return ((jnp.cos(phase_angle) + jnp.sin(phase_angle)) / math.sqrt(length)).astype(jnp.bfloat16)


def step_embedding(noise_step, channel, channels):
    half_count = channels // 2
    lower_half = channel < half_count
    position = jnp.where(lower_half, channel, channel - half_count).astype(jnp.float32)
    frequency = jnp.exp(-math.log(10000.0) * position / half_count)
    phase_angle = noise_step[0].astype(jnp.float32) * frequency
    return jnp.where(lower_half, jnp.sin(phase_angle), jnp.cos(phase_angle))


def apply_table(form, table, operand):
    return jnp.einsum(form, table, operand, preferred_element_type=jnp.float32)


def local_split_channels(latents, spectrum, w_value, w_gate, w_out, embed_table, prompt_ids, noise_step):
    row_count = latents.shape[0]
    chan_part = w_value.shape[1]
    full_value, full_gate, full_out = (
        lax.all_gather(w_value, "sp", axis=0, tiled=True),
        lax.all_gather(w_gate, "sp", axis=0, tiled=True),
        lax.all_gather(w_out, "sp", axis=0, tiled=True),
    )
    value_rows = jnp.dot(latents, full_value, preferred_element_type=jnp.float32).astype(
        jnp.bfloat16
    )
    gate_rows = jnp.dot(latents, full_gate, preferred_element_type=jnp.float32)
    cas_width = cas_table(WW)
    cas_height = cas_table(HH)
    cas_time = cas_table(TT)
    line_grid = value_rows.reshape(row_count // WW, WW, chan_part)
    width_spec = apply_table("kw,lwc->lkc", cas_width, line_grid).astype(jnp.bfloat16)
    pencil = lax.all_to_all(width_spec, "sp", split_axis=1, concat_axis=0, tiled=True)
    band_count = pencil.shape[1]
    pencil = pencil.reshape(TT, HH, band_count, chan_part)
    height_spec = apply_table("ah,thkc->takc", cas_height, pencil).astype(jnp.bfloat16)
    full_spec = apply_table("st,takc->sakc", cas_time, height_spec).astype(jnp.bfloat16)
    filtered = (full_spec.astype(jnp.float32) * spectrum.astype(jnp.float32)).astype(jnp.bfloat16)
    time_back = apply_table("ts,sakc->takc", cas_time, filtered).astype(jnp.bfloat16)
    height_back = apply_table("ha,takc->thkc", cas_height, time_back).astype(jnp.bfloat16)
    returned = lax.all_to_all(
        height_back.reshape(TT * HH, band_count, chan_part),
        "sp",
        split_axis=0,
        concat_axis=1,
        tiled=True,
    )
    mix_rows = apply_table("wk,lkc->lwc", cas_width, returned).reshape(row_count, chan_part)
    offset = lax.axis_index("ch") * chan_part
    local_pool = jnp.mean(jnp.take(embed_table, prompt_ids, axis=1).astype(jnp.float32), axis=1)
    pooled_all = lax.all_gather(local_pool, ("sp", "ch"), axis=0, tiled=True)
    pooled = lax.dynamic_slice_in_dim(pooled_all, offset, chan_part)
    channel = offset + jnp.arange(chan_part, dtype=jnp.int32)
    modulation = 1.0 + pooled + step_embedding(noise_step, channel, C)
    mixed_rows = (mix_rows * jax.nn.silu(gate_rows) * modulation[None, :]).astype(jnp.bfloat16)
    half_rows = row_count // lax.axis_size("ch")
    own_rows = lax.dynamic_slice_in_dim(full_out, offset, chan_part, 0)
    summed = lax.psum_scatter(
        jnp.dot(mixed_rows, own_rows, preferred_element_type=jnp.float32).astype(jnp.bfloat16),
        "ch",
        scatter_dimension=0,
        tiled=True,
    ).astype(jnp.float32)
    residual = lax.dynamic_slice_in_dim(latents, lax.axis_index("ch") * half_rows, half_rows, 0)
    return (residual.astype(jnp.float32) + summed).astype(jnp.bfloat16)


SUB = 8
MIB = 1 << 20


def cas_host(length):
    position = np.arange(length)
    phase_angle = (position[:, None] * position[None, :] % length).astype(np.float32) * np.float32(
        2.0 * math.pi / length
    )
    table = (np.cos(phase_angle) + np.sin(phase_angle)) / np.float32(math.sqrt(length))
    return table.astype(jnp.bfloat16).astype(np.float32)


def width_table(devices, band_count, bands):
    frequency = (np.arange(devices)[:, None] * band_count + np.asarray(bands)[None, :]).reshape(-1)
    rows = cas_host(WW)[frequency]
    return np.einsum("fw,lm->flmw", rows, np.eye(SUB, dtype=np.float32)).reshape(
        len(frequency) * SUB, SUB * WW
    ).astype(jnp.bfloat16)


def plane_table():
    return np.kron(cas_host(TT), cas_host(HH)).astype(jnp.bfloat16)


def dot32(left, right, contract=(1, 0)):
    return lax.dot_general(
        left, right, (((contract[0],), (contract[1],)), ((), ())), preferred_element_type=jnp.float32
    )


def forward_body(table_ref, rows_ref, out_ref):
    spec = dot32(table_ref[...], rows_ref[...])
    out_ref[...] = spec.reshape(out_ref.shape).astype(jnp.bfloat16)


def kernel_params(axes):
    return pltpu.CompilerParams(
        dimension_semantics=("arbitrary",) * axes, vmem_limit_bytes=58 * MIB
    )


def width_forward(table, latents, devices, bands):
    rows, chans = latents.shape
    group = SUB * WW
    lines = rows // WW
    return pl.pallas_call(
        forward_body,
        name="width_forward",
        grid=(rows // group,),
        in_specs=[
            pl.BlockSpec(table.shape, lambda g: (0, 0)),
            pl.BlockSpec((group, chans), lambda g: (g, 0)),
        ],
        out_specs=pl.BlockSpec((devices, bands, SUB, chans), lambda g: (0, 0, g, 0)),
        out_shape=jax.ShapeDtypeStruct((devices, bands, lines, chans), jnp.bfloat16),
        compiler_params=kernel_params(1),
        cost_estimate=pl.CostEstimate(
            flops=2 * rows * chans * table.shape[0],
            bytes_accessed=4 * rows * chans,
            transcendentals=0,
        ),
    )(table, latents)


def plane_body(table_ref, value_ref, spectrum_ref, pencil_ref, *rest):
    out_refs, (first_ref, second_ref) = rest[:-2], rest[-2:]
    cells, chans = first_ref.shape
    step = min(cells, 256)
    lines = pencil_ref.shape[2]
    pencil = pencil_ref[...].reshape(cells, chans)
    for at in range(0, cells, step):
        part = pl.ds(at, step)
        first_ref[part, :] = dot32(table_ref[part, :], pencil).astype(jnp.bfloat16)
    for at in range(0, cells, step):
        part = pl.ds(at, step)
        full = dot32(first_ref[part, :], value_ref[...])
        gain = spectrum_ref[0, part, :].astype(jnp.float32)
        second_ref[part, :] = (full * gain).astype(jnp.bfloat16)
    per = step // lines
    for at in range(0, cells, step):
        back = dot32(table_ref[pl.ds(at, step), :], second_ref[...])
        back = back.reshape(per, lines, chans).astype(jnp.bfloat16)
        line = 0
        for out_ref in out_refs:
            count = out_ref.shape[2]
            out_ref[pl.ds(at // lines, per), 0] = back[:, line : line + count]
            line += count


def plane_filter(table, w_value, spectrum, pencil, first_band, splits):
    devices, bands, lines, chans = pencil.shape
    cells = devices * lines
    block = lambda count: pl.BlockSpec((devices, 1, count, chans), lambda j: (0, j, 0, 0))
    return pl.pallas_call(
        plane_body,
        name="plane_filter",
        grid=(bands,),
        in_specs=[
            pl.BlockSpec(table.shape, lambda j: (0, 0)),
            pl.BlockSpec(w_value.shape, lambda j: (0, 0)),
            pl.BlockSpec((1, cells, chans), lambda j: (first_band + j, 0, 0)),
            block(lines),
        ],
        out_specs=[block(count) for count in splits],
        out_shape=[
            jax.ShapeDtypeStruct((devices, bands, count, chans), jnp.bfloat16) for count in splits
        ],
        scratch_shapes=[pltpu.VMEM((cells, chans), jnp.bfloat16)] * 2,
        compiler_params=kernel_params(1),
        cost_estimate=pl.CostEstimate(
            flops=2 * bands * cells * chans * (2 * cells + chans),
            bytes_accessed=6 * bands * cells * chans,
            transcendentals=0,
        ),
    )(table, w_value, spectrum, pencil)


def finish_body(parts, *refs):
    tables, spectra = refs[:parts], refs[parts : 2 * parts]
    gate_ref, latents_ref, w_out_ref = refs[2 * parts : 2 * parts + 3]
    out_ref, spec_refs = refs[-1 - parts], refs[-parts:]

    @pl.when(pl.program_id(1) == 0)
    def _():
        for source, held in zip(spectra, spec_refs):
            wide = source[...].astype(jnp.float32).reshape(held.shape)
            held[...] = wide.astype(jnp.bfloat16)

    mix = None
    for table_ref, held in zip(tables, spec_refs):
        term = dot32(table_ref[...], held[...], (0, 0))
        mix = term if mix is None else mix + term
    mixed = (mix * gate_ref[...].astype(jnp.float32)).astype(jnp.bfloat16)
    out = latents_ref[...].astype(jnp.float32) + dot32(mixed, w_out_ref[...])
    out_ref[...] = out.astype(jnp.bfloat16)


def finish(tables, spectra, starts, gate, latents, w_out, groups, done=None):
    rows, chans = latents.shape
    group = SUB * WW
    first, count = groups
    pieces = 4
    piece = group // pieces
    by_piece = pl.BlockSpec((piece, chans), lambda g, s: ((first + g) * pieces + s, 0))
    spec_block = lambda spec, start: pl.BlockSpec(
        spec.shape[:2] + (SUB, chans), lambda g, s: (0, 0, first + g - start, 0)
    )
    inputs = [*tables, *spectra, gate, latents, w_out] + ([] if done is None else [done])
    return pl.pallas_call(
        functools.partial(finish_body, len(tables)),
        name="finish",
        grid=(count, pieces),
        in_specs=[
            pl.BlockSpec((table.shape[0], piece), lambda g, s: (0, s)) for table in tables
        ]
        + [spec_block(spec, start) for spec, start in zip(spectra, starts)]
        + [by_piece, by_piece, pl.BlockSpec(w_out.shape, lambda g, s: (0, 0))]
        + ([] if done is None else [pl.BlockSpec(memory_space=pl.ANY)]),
        out_specs=by_piece,
        out_shape=jax.ShapeDtypeStruct((rows, chans), jnp.bfloat16),
        scratch_shapes=[pltpu.VMEM((table.shape[0], chans), jnp.bfloat16) for table in tables],
        input_output_aliases={} if done is None else {len(inputs) - 1: 0},
        compiler_params=kernel_params(2),
        cost_estimate=pl.CostEstimate(
            flops=2 * count * group * chans * (group + chans),
            bytes_accessed=8 * count * group * chans,
            transcendentals=0,
        ),
    )(*inputs)


def exchange(tensor):
    return lax.all_to_all(tensor, "sp", split_axis=0, concat_axis=0, tiled=True)


def spread(held, bits, devices):
    deltas = [0]
    for bit in bits:
        deltas = deltas + [delta ^ bit for delta in deltas]
    blocks = [held]
    for delta in deltas[1:]:
        pairs = [(i, i ^ delta) for i in range(devices)]
        blocks.append(lax.ppermute(held, "sp", pairs))
    return blocks, deltas


def gather_blocks(block, stages, devices):
    order = [0]
    held = block[None]
    for bits in stages:
        blocks, deltas = spread(held, bits, devices)
        held = jnp.concatenate(blocks, axis=0)
        order = [slot ^ delta for delta in deltas for slot in order]
    slot_of = jnp.asarray(np.argsort(np.asarray(order)), jnp.int32)
    own = lax.axis_index("sp")
    slots = slot_of[jnp.arange(devices, dtype=jnp.int32) ^ own]
    return jnp.take(held, slots, axis=0)


def gather_stages(devices):
    bits = [1 << at for at in range(devices.bit_length() - 1)]
    return [stage for stage in (bits[3:], bits[1:3], bits[:1]) if stage]


def chunks_of(band_count):
    return [(0,)] + ([tuple(range(1, band_count))] if band_count > 1 else [])


def splits_of(lines):
    return [lines - SUB, SUB] if lines > SUB else [lines]


def local_planes(devices, *args):
    return planes(devices, *args)


def planes(devices, latents, spectrum, w_value, w_gate, w_out, embed_table, prompt_ids, noise_step):
    row_count, chans = latents.shape
    band_count = spectrum.shape[2]
    lines = row_count // WW
    chunks = chunks_of(band_count)
    splits = splits_of(lines)
    stages = gather_stages(devices)
    tables = [jnp.asarray(width_table(devices, band_count, bands)) for bands in chunks]
    plane = jnp.asarray(plane_table())
    per = w_value.shape[0]

    pencils = []
    for table, bands in zip(tables, chunks):
        part = width_forward(table, latents, devices, len(bands))
        pencils.append(exchange(part))

    both = gather_blocks(jnp.concatenate([w_value, w_gate], axis=0), stages, devices)
    full_value = both[:, :per].reshape(-1, chans)
    full_gate = both[:, per:].reshape(-1, chans)

    taken = jnp.take(embed_table, prompt_ids, axis=1).astype(jnp.float32)
    pooled = jnp.mean(taken, axis=1)
    channel = lax.axis_index("sp") * per + jnp.arange(per, dtype=jnp.int32)
    modulation = 1.0 + pooled + step_embedding(noise_step, channel, chans)
    scaled = (w_out.astype(jnp.float32) * modulation[:, None]).astype(jnp.bfloat16)
    full_out = gather_blocks(scaled, stages, devices).reshape(-1, chans)

    gain = spectrum.transpose(2, 0, 1, 3).reshape(band_count, TT * HH, chans)

    returned = []
    for at, (pencil, bands) in enumerate(zip(pencils, chunks)):
        last = at == len(chunks) - 1
        parts = plane_filter(plane, full_value, gain, pencil, bands[0], splits if last else [lines])
        returned.append([exchange(part) for part in parts])

    gate_rows = jnp.dot(latents, full_gate, preferred_element_type=jnp.float32)
    gate = jax.nn.silu(gate_rows).astype(jnp.bfloat16)

    done, line = None, 0
    for piece, count in enumerate(splits):
        spectra = [back[min(piece, len(back) - 1)] for back in returned]
        starts = [0 if len(back) == 1 else line // SUB for back in returned]
        done = finish(
            tables, spectra, starts, gate, latents, full_out,
            (line // SUB, count // SUB), done,
        )
        line += count
    return done


def solution(mesh):
    placed = (
        P(("grp", "sp"), None),
        P(None, None, "sp", "ch"),
        P("sp", "ch"),
        P("sp", "ch"),
        P("sp", None),
        P(("sp", "ch"), None),
        P("grp"),
        P("grp"),
    )
    devices = mesh.shape["sp"]
    lines = TT * HH // devices
    whole_channels = mesh.shape["ch"] == 1 and devices & (devices - 1) == 0 and lines % SUB == 0
    local = functools.partial(local_planes, devices) if whole_channels else local_split_channels
    return jax.shard_map(
        local, mesh=mesh, in_specs=placed, out_specs=P(("grp", "sp", "ch"), None), check_vma=False
    )
```

```python
import functools
import math

import jax
import jax.numpy as jnp
import numpy as np
from jax import lax
from jax.experimental import pallas as pl
from jax.experimental.pallas import tpu as pltpu
from jax.sharding import PartitionSpec as P


TT = 16
HH = 64
WW = 128
C = 1024


def cas_table(length):
    position = jnp.arange(length, dtype=jnp.int32)
    product = position[:, None] * position[None, :] % length
    phase_angle = product.astype(jnp.float32) * (2.0 * math.pi / length)
    return ((jnp.cos(phase_angle) + jnp.sin(phase_angle)) / math.sqrt(length)).astype(jnp.bfloat16)


def step_embedding(noise_step, channel, channels):
    half_count = channels // 2
    lower_half = channel < half_count
    position = jnp.where(lower_half, channel, channel - half_count).astype(jnp.float32)
    frequency = jnp.exp(-math.log(10000.0) * position / half_count)
    phase_angle = noise_step[0].astype(jnp.float32) * frequency
    return jnp.where(lower_half, jnp.sin(phase_angle), jnp.cos(phase_angle))


def apply_table(form, table, operand):
    return jnp.einsum(form, table, operand, preferred_element_type=jnp.float32)


def local_split_channels(latents, spectrum, w_value, w_gate, w_out, embed_table, prompt_ids, noise_step):
    row_count = latents.shape[0]
    chan_part = w_value.shape[1]
    full_value, full_gate, full_out = (
        lax.all_gather(w_value, "sp", axis=0, tiled=True),
        lax.all_gather(w_gate, "sp", axis=0, tiled=True),
        lax.all_gather(w_out, "sp", axis=0, tiled=True),
    )
    value_rows = jnp.dot(latents, full_value, preferred_element_type=jnp.float32).astype(
        jnp.bfloat16
    )
    gate_rows = jnp.dot(latents, full_gate, preferred_element_type=jnp.float32)
    cas_width = cas_table(WW)
    cas_height = cas_table(HH)
    cas_time = cas_table(TT)
    line_grid = value_rows.reshape(row_count // WW, WW, chan_part)
    width_spec = apply_table("kw,lwc->lkc", cas_width, line_grid).astype(jnp.bfloat16)
    pencil = lax.all_to_all(width_spec, "sp", split_axis=1, concat_axis=0, tiled=True)
    band_count = pencil.shape[1]
    pencil = pencil.reshape(TT, HH, band_count, chan_part)
    height_spec = apply_table("ah,thkc->takc", cas_height, pencil).astype(jnp.bfloat16)
    full_spec = apply_table("st,takc->sakc", cas_time, height_spec).astype(jnp.bfloat16)
    filtered = (full_spec.astype(jnp.float32) * spectrum.astype(jnp.float32)).astype(jnp.bfloat16)
    time_back = apply_table("ts,sakc->takc", cas_time, filtered).astype(jnp.bfloat16)
    height_back = apply_table("ha,takc->thkc", cas_height, time_back).astype(jnp.bfloat16)
    returned = lax.all_to_all(
        height_back.reshape(TT * HH, band_count, chan_part),
        "sp",
        split_axis=0,
        concat_axis=1,
        tiled=True,
    )
    mix_rows = apply_table("wk,lkc->lwc", cas_width, returned).reshape(row_count, chan_part)
    offset = lax.axis_index("ch") * chan_part
    local_pool = jnp.mean(jnp.take(embed_table, prompt_ids, axis=1).astype(jnp.float32), axis=1)
    pooled_all = lax.all_gather(local_pool, ("sp", "ch"), axis=0, tiled=True)
    pooled = lax.dynamic_slice_in_dim(pooled_all, offset, chan_part)
    channel = offset + jnp.arange(chan_part, dtype=jnp.int32)
    modulation = 1.0 + pooled + step_embedding(noise_step, channel, C)
    mixed_rows = (mix_rows * jax.nn.silu(gate_rows) * modulation[None, :]).astype(jnp.bfloat16)
    half_rows = row_count // lax.axis_size("ch")
    own_rows = lax.dynamic_slice_in_dim(full_out, offset, chan_part, 0)
    summed = lax.psum_scatter(
        jnp.dot(mixed_rows, own_rows, preferred_element_type=jnp.float32).astype(jnp.bfloat16),
        "ch",
        scatter_dimension=0,
        tiled=True,
    ).astype(jnp.float32)
    residual = lax.dynamic_slice_in_dim(latents, lax.axis_index("ch") * half_rows, half_rows, 0)
    return (residual.astype(jnp.float32) + summed).astype(jnp.bfloat16)


SUB = 8
MIB = 1 << 20


def cas_host(length):
    position = np.arange(length)
    phase_angle = (position[:, None] * position[None, :] % length).astype(np.float32) * np.float32(
        2.0 * math.pi / length
    )
    table = (np.cos(phase_angle) + np.sin(phase_angle)) / np.float32(math.sqrt(length))
    return table.astype(jnp.bfloat16).astype(np.float32)


def width_table(devices, band_count, bands):
    frequency = (np.arange(devices)[:, None] * band_count + np.asarray(bands)[None, :]).reshape(-1)
    rows = cas_host(WW)[frequency]
    return np.einsum("fw,lm->flmw", rows, np.eye(SUB, dtype=np.float32)).reshape(
        len(frequency) * SUB, SUB * WW
    ).astype(jnp.bfloat16)


def plane_table():
    return np.kron(cas_host(TT), cas_host(HH)).astype(jnp.bfloat16)


def dot32(left, right, contract=(1, 0)):
    return lax.dot_general(
        left, right, (((contract[0],), (contract[1],)), ((), ())), preferred_element_type=jnp.float32
    )


def forward_body(table_ref, rows_ref, out_ref):
    spec = dot32(table_ref[...], rows_ref[...])
    out_ref[...] = spec.reshape(out_ref.shape).astype(jnp.bfloat16)


def kernel_params(axes, mib=58):
    return pltpu.CompilerParams(
        dimension_semantics=("arbitrary",) * axes, vmem_limit_bytes=mib * MIB
    )


def width_forward(table, latents, devices, bands):
    rows, chans = latents.shape
    group = SUB * WW
    lines = rows // WW
    return pl.pallas_call(
        forward_body,
        name="width_forward",
        grid=(rows // group,),
        in_specs=[
            pl.BlockSpec(table.shape, lambda g: (0, 0)),
            pl.BlockSpec((group, chans), lambda g: (g, 0)),
        ],
        out_specs=pl.BlockSpec((devices, bands, SUB, chans), lambda g: (0, 0, g, 0)),
        out_shape=jax.ShapeDtypeStruct((devices, bands, lines, chans), jnp.bfloat16),
        compiler_params=kernel_params(1),
        cost_estimate=pl.CostEstimate(
            flops=2 * rows * chans * table.shape[0],
            bytes_accessed=4 * rows * chans,
            transcendentals=0,
        ),
    )(table, latents)


def plane_body(table_ref, value_ref, spectrum_ref, pencil_ref, *rest):
    out_refs, (first_ref, second_ref) = rest[:-2], rest[-2:]
    cells, chans = first_ref.shape
    step = min(cells, 256)
    lines = pencil_ref.shape[2]
    pencil = pencil_ref[...].reshape(cells, chans)
    for at in range(0, cells, step):
        part = pl.ds(at, step)
        first_ref[part, :] = dot32(table_ref[part, :], pencil).astype(jnp.bfloat16)
    for at in range(0, cells, step):
        part = pl.ds(at, step)
        full = dot32(first_ref[part, :], value_ref[...])
        gain = spectrum_ref[0, part, :].astype(jnp.float32)
        second_ref[part, :] = (full * gain).astype(jnp.bfloat16)
    per = step // lines
    for at in range(0, cells, step):
        back = dot32(table_ref[pl.ds(at, step), :], second_ref[...])
        back = back.reshape(per, lines, chans).astype(jnp.bfloat16)
        line = 0
        for out_ref in out_refs:
            count = out_ref.shape[2]
            out_ref[pl.ds(at // lines, per), 0] = back[:, line : line + count]
            line += count


def plane_filter(table, w_value, spectrum, pencil, first_band, splits):
    devices, bands, lines, chans = pencil.shape
    cells = devices * lines
    block = lambda count: pl.BlockSpec((devices, 1, count, chans), lambda j: (0, j, 0, 0))
    return pl.pallas_call(
        plane_body,
        name="plane_filter",
        grid=(bands,),
        in_specs=[
            pl.BlockSpec(table.shape, lambda j: (0, 0)),
            pl.BlockSpec(w_value.shape, lambda j: (0, 0)),
            pl.BlockSpec((1, cells, chans), lambda j: (first_band + j, 0, 0)),
            block(lines),
        ],
        out_specs=[block(count) for count in splits],
        out_shape=[
            jax.ShapeDtypeStruct((devices, bands, count, chans), jnp.bfloat16) for count in splits
        ],
        scratch_shapes=[pltpu.VMEM((cells, chans), jnp.bfloat16)] * 2,
        compiler_params=kernel_params(1),
        cost_estimate=pl.CostEstimate(
            flops=2 * bands * cells * chans * (2 * cells + chans),
            bytes_accessed=6 * bands * cells * chans,
            transcendentals=0,
        ),
    )(table, w_value, spectrum, pencil)


def finish_body(parts, *refs):
    tables, spectra = refs[:parts], refs[parts : 2 * parts]
    gate_ref, latents_ref, w_out_ref = refs[2 * parts : 2 * parts + 3]
    out_ref, spec_refs = refs[-1 - parts], refs[-parts:]

    @pl.when(pl.program_id(1) == 0)
    def _():
        for source, held in zip(spectra, spec_refs):
            wide = source[...].astype(jnp.float32).reshape(held.shape)
            held[...] = wide.astype(jnp.bfloat16)

    mix = None
    for table_ref, held in zip(tables, spec_refs):
        term = dot32(table_ref[...], held[...], (0, 0))
        mix = term if mix is None else mix + term
    mixed = (mix * gate_ref[...].astype(jnp.float32)).astype(jnp.bfloat16)
    out = latents_ref[...].astype(jnp.float32) + dot32(mixed, w_out_ref[...])
    out_ref[...] = out.astype(jnp.bfloat16)


def finish(tables, spectra, starts, gate, latents, w_out, groups, done=None):
    rows, chans = latents.shape
    group = SUB * WW
    first, count = groups
    pieces = 4
    piece = group // pieces
    by_piece = pl.BlockSpec((piece, chans), lambda g, s: ((first + g) * pieces + s, 0))
    spec_block = lambda spec, start: pl.BlockSpec(
        spec.shape[:2] + (SUB, chans), lambda g, s: (0, 0, first + g - start, 0)
    )
    inputs = [*tables, *spectra, gate, latents, w_out] + ([] if done is None else [done])
    return pl.pallas_call(
        functools.partial(finish_body, len(tables)),
        name="finish",
        grid=(count, pieces),
        in_specs=[
            pl.BlockSpec((table.shape[0], piece), lambda g, s: (0, s)) for table in tables
        ]
        + [spec_block(spec, start) for spec, start in zip(spectra, starts)]
        + [by_piece, by_piece, pl.BlockSpec(w_out.shape, lambda g, s: (0, 0))]
        + ([] if done is None else [pl.BlockSpec(memory_space=pl.ANY)]),
        out_specs=by_piece,
        out_shape=jax.ShapeDtypeStruct((rows, chans), jnp.bfloat16),
        scratch_shapes=[pltpu.VMEM((table.shape[0], chans), jnp.bfloat16) for table in tables],
        input_output_aliases={} if done is None else {len(inputs) - 1: 0},
        compiler_params=kernel_params(2),
        cost_estimate=pl.CostEstimate(
            flops=2 * count * group * chans * (group + chans),
            bytes_accessed=8 * count * group * chans,
            transcendentals=0,
        ),
    )(*inputs)


def exchange(tensor):
    return lax.all_to_all(tensor, "sp", split_axis=0, concat_axis=0, tiled=True)


def combinations(bits):
    deltas = [0]
    for bit in bits:
        deltas = deltas + [delta ^ bit for delta in deltas]
    return deltas


def spread(held, bits, devices):
    blocks = [held]
    for delta in combinations(bits)[1:]:
        pairs = [(i, i ^ delta) for i in range(devices)]
        blocks.append(lax.ppermute(held, "sp", pairs))
    return blocks


def gather_stages(devices):
    bits = [1 << at for at in range(devices.bit_length() - 1)]
    return [bits[3:], bits[1:3], bits[:1]]


def in_order(blocks, stages, devices):
    order = [0]
    for bits in stages:
        order = [slot ^ delta for delta in combinations(bits) for slot in order]
    slot_of = jnp.asarray(np.argsort(np.asarray(order)), jnp.int32)
    own = lax.axis_index("sp")
    slots = slot_of[jnp.arange(devices, dtype=jnp.int32) ^ own]
    held = jnp.concatenate(blocks, axis=0)
    held = held.at[slots].get(mode="promise_in_bounds", wrap_negative_indices=False)
    return held.reshape(-1, held.shape[-1])


def chunks_of(band_count):
    return [(0,)] + ([tuple(range(1, band_count))] if band_count > 1 else [])


def splits_of(lines):
    return [lines - SUB, SUB] if lines > SUB else [lines]


def local_planes(devices, *args):
    return planes(devices, *args)


def planes(devices, latents, spectrum, w_value, w_gate, w_out, embed_table, prompt_ids, noise_step):
    row_count, chans = latents.shape
    band_count = spectrum.shape[2]
    lines = row_count // WW
    chunks = chunks_of(band_count)
    splits = splits_of(lines)
    stages = gather_stages(devices)
    tables = [jnp.asarray(width_table(devices, band_count, bands)) for bands in chunks]
    plane = jnp.asarray(plane_table())
    per = w_value.shape[0]

    pencils = []
    for table, bands in zip(tables, chunks):
        part = width_forward(table, latents, devices, len(bands))
        pencils.append(exchange(part))

    def joined(blocks, stage):
        return spread(jnp.concatenate(blocks, axis=0), stages[stage], devices)

    value_blocks = spread(w_value[None], stages[0], devices)
    for stage in (1, 2):
        value_blocks = joined(value_blocks, stage)
    full_value = in_order(value_blocks, stages, devices)

    gate_blocks = spread(w_gate[None], stages[0], devices)
    gate_blocks = joined(gate_blocks, 1)

    taken = jnp.take(embed_table, prompt_ids, axis=1).astype(jnp.float32)
    pooled = jnp.mean(taken, axis=1)
    channel = lax.axis_index("sp") * per + jnp.arange(per, dtype=jnp.int32)
    modulation = 1.0 + pooled + step_embedding(noise_step, channel, chans)
    scaled = (w_out.astype(jnp.float32) * modulation[:, None]).astype(jnp.bfloat16)
    out_blocks = spread(scaled[None], stages[0], devices)
    out_blocks, gate_blocks = lax.optimization_barrier((out_blocks, gate_blocks))
    full_gate = in_order(joined(gate_blocks, 2), stages, devices)
    for stage in (1, 2):
        out_blocks = joined(out_blocks, stage)
    full_out = in_order(out_blocks, stages, devices)

    gain = spectrum.transpose(2, 0, 1, 3).reshape(band_count, TT * HH, chans)

    returned = []
    for at, (pencil, bands) in enumerate(zip(pencils, chunks)):
        last = at == len(chunks) - 1
        parts = plane_filter(plane, full_value, gain, pencil, bands[0], splits if last else [lines])
        returned.append([exchange(part) for part in parts])

    gate_rows = jnp.dot(latents, full_gate, preferred_element_type=jnp.float32)
    gate = jax.nn.silu(gate_rows).astype(jnp.bfloat16)

    done, line = None, 0
    for piece, count in enumerate(splits):
        spectra = [back[min(piece, len(back) - 1)] for back in returned]
        starts = [0 if len(back) == 1 else line // SUB for back in returned]
        done = finish(
            tables, spectra, starts, gate, latents, full_out,
            (line // SUB, count // SUB), done,
        )
        line += count
    return done


def solution(mesh):
    placed = (
        P(("grp", "sp"), None),
        P(None, None, "sp", "ch"),
        P("sp", "ch"),
        P("sp", "ch"),
        P("sp", None),
        P(("sp", "ch"), None),
        P("grp"),
        P("grp"),
    )
    devices = mesh.shape["sp"]
    lines = TT * HH // devices
    whole_channels = mesh.shape["ch"] == 1 and devices & (devices - 1) == 0 and lines % SUB == 0
    local = functools.partial(local_planes, devices) if whole_channels else local_split_channels
    return jax.shard_map(
        local, mesh=mesh, in_specs=placed, out_specs=P(("grp", "sp", "ch"), None), check_vma=False
    )
```

```python
import functools
import math

import jax
import jax.numpy as jnp
import numpy as np
from jax import lax
from jax.experimental import pallas as pl
from jax.experimental.pallas import tpu as pltpu
from jax.sharding import PartitionSpec as P


TT = 16
HH = 64
WW = 128
C = 1024


def cas_table(length):
    position = jnp.arange(length, dtype=jnp.int32)
    product = position[:, None] * position[None, :] % length
    phase_angle = product.astype(jnp.float32) * (2.0 * math.pi / length)
    return ((jnp.cos(phase_angle) + jnp.sin(phase_angle)) / math.sqrt(length)).astype(jnp.bfloat16)


def step_embedding(noise_step, channel, channels):
    half_count = channels // 2
    lower_half = channel < half_count
    position = jnp.where(lower_half, channel, channel - half_count).astype(jnp.float32)
    frequency = jnp.exp(-math.log(10000.0) * position / half_count)
    phase_angle = noise_step[0].astype(jnp.float32) * frequency
    return jnp.where(lower_half, jnp.sin(phase_angle), jnp.cos(phase_angle))


def apply_table(form, table, operand):
    return jnp.einsum(form, table, operand, preferred_element_type=jnp.float32)


def local_split_channels(latents, spectrum, w_value, w_gate, w_out, embed_table, prompt_ids, noise_step):
    row_count = latents.shape[0]
    chan_part = w_value.shape[1]
    full_value, full_gate, full_out = (
        lax.all_gather(w_value, "sp", axis=0, tiled=True),
        lax.all_gather(w_gate, "sp", axis=0, tiled=True),
        lax.all_gather(w_out, "sp", axis=0, tiled=True),
    )
    value_rows = jnp.dot(latents, full_value, preferred_element_type=jnp.float32).astype(
        jnp.bfloat16
    )
    gate_rows = jnp.dot(latents, full_gate, preferred_element_type=jnp.float32)
    cas_width = cas_table(WW)
    cas_height = cas_table(HH)
    cas_time = cas_table(TT)
    line_grid = value_rows.reshape(row_count // WW, WW, chan_part)
    width_spec = apply_table("kw,lwc->lkc", cas_width, line_grid).astype(jnp.bfloat16)
    pencil = lax.all_to_all(width_spec, "sp", split_axis=1, concat_axis=0, tiled=True)
    band_count = pencil.shape[1]
    pencil = pencil.reshape(TT, HH, band_count, chan_part)
    height_spec = apply_table("ah,thkc->takc", cas_height, pencil).astype(jnp.bfloat16)
    full_spec = apply_table("st,takc->sakc", cas_time, height_spec).astype(jnp.bfloat16)
    filtered = (full_spec.astype(jnp.float32) * spectrum.astype(jnp.float32)).astype(jnp.bfloat16)
    time_back = apply_table("ts,sakc->takc", cas_time, filtered).astype(jnp.bfloat16)
    height_back = apply_table("ha,takc->thkc", cas_height, time_back).astype(jnp.bfloat16)
    returned = lax.all_to_all(
        height_back.reshape(TT * HH, band_count, chan_part),
        "sp",
        split_axis=0,
        concat_axis=1,
        tiled=True,
    )
    mix_rows = apply_table("wk,lkc->lwc", cas_width, returned).reshape(row_count, chan_part)
    offset = lax.axis_index("ch") * chan_part
    local_pool = jnp.mean(jnp.take(embed_table, prompt_ids, axis=1).astype(jnp.float32), axis=1)
    pooled_all = lax.all_gather(local_pool, ("sp", "ch"), axis=0, tiled=True)
    pooled = lax.dynamic_slice_in_dim(pooled_all, offset, chan_part)
    channel = offset + jnp.arange(chan_part, dtype=jnp.int32)
    modulation = 1.0 + pooled + step_embedding(noise_step, channel, C)
    mixed_rows = (mix_rows * jax.nn.silu(gate_rows) * modulation[None, :]).astype(jnp.bfloat16)
    half_rows = row_count // lax.axis_size("ch")
    own_rows = lax.dynamic_slice_in_dim(full_out, offset, chan_part, 0)
    summed = lax.psum_scatter(
        jnp.dot(mixed_rows, own_rows, preferred_element_type=jnp.float32).astype(jnp.bfloat16),
        "ch",
        scatter_dimension=0,
        tiled=True,
    ).astype(jnp.float32)
    residual = lax.dynamic_slice_in_dim(latents, lax.axis_index("ch") * half_rows, half_rows, 0)
    return (residual.astype(jnp.float32) + summed).astype(jnp.bfloat16)


SUB = 8
NEAR = 8
MIB = 1 << 20


def cas_host(length):
    position = np.arange(length)
    phase_angle = (position[:, None] * position[None, :] % length).astype(np.float32) * np.float32(
        2.0 * math.pi / length
    )
    table = (np.cos(phase_angle) + np.sin(phase_angle)) / np.float32(math.sqrt(length))
    return table.astype(jnp.bfloat16).astype(np.float32)


def width_table(devices, band_count, bands):
    frequency = (np.arange(devices)[:, None] * band_count + np.asarray(bands)[None, :]).reshape(-1)
    rows = cas_host(WW)[frequency]
    return np.einsum("fw,lm->flmw", rows, np.eye(SUB, dtype=np.float32)).reshape(
        len(frequency) * SUB, SUB * WW
    ).astype(jnp.bfloat16)


def plane_table():
    return np.kron(cas_host(TT), cas_host(HH)).astype(jnp.bfloat16)


def dot32(left, right, contract=(1, 0)):
    return lax.dot_general(
        left, right, (((contract[0],), (contract[1],)), ((), ())), preferred_element_type=jnp.float32
    )


def forward_body(table_ref, rows_ref, out_ref):
    spec = dot32(table_ref[...], rows_ref[...])
    out_ref[...] = spec.reshape(out_ref.shape).astype(jnp.bfloat16)


def kernel_params(axes):
    return pltpu.CompilerParams(
        dimension_semantics=("arbitrary",) * axes, vmem_limit_bytes=58 * MIB
    )


def width_forward(table, latents, devices, bands):
    rows, chans = latents.shape
    group = SUB * WW
    lines = rows // WW
    return pl.pallas_call(
        forward_body,
        name="width_forward",
        grid=(rows // group,),
        in_specs=[
            pl.BlockSpec(table.shape, lambda g: (0, 0)),
            pl.BlockSpec((group, chans), lambda g: (g, 0)),
        ],
        out_specs=pl.BlockSpec((devices, bands, SUB, chans), lambda g: (0, 0, g, 0)),
        out_shape=jax.ShapeDtypeStruct((devices, bands, lines, chans), jnp.bfloat16),
        compiler_params=kernel_params(1),
        cost_estimate=pl.CostEstimate(
            flops=2 * rows * chans * table.shape[0],
            bytes_accessed=4 * rows * chans,
            transcendentals=0,
        ),
    )(table, latents)


def plane_body(own_ref, table_ref, value_ref, spectrum_ref, pencil_ref, *rest):
    out_refs, (first_ref, second_ref) = rest[:-2], rest[-2:]
    cells, chans = first_ref.shape
    lines = pencil_ref.shape[2]
    step = NEAR * lines
    pencil = pencil_ref[...].reshape(cells, chans)
    for at in range(0, cells, step):
        part = pl.ds(at, step)
        first_ref[part, :] = dot32(table_ref[part, :], pencil).astype(jnp.bfloat16)
    for at in range(0, cells, step):
        part = pl.ds(at, step)
        full = dot32(first_ref[part, :], value_ref[...])
        gain = spectrum_ref[0, part, :].astype(jnp.float32)
        second_ref[part, :] = (full * gain).astype(jnp.bfloat16)
    keep = out_refs[0].shape[2]
    for plane in range(cells // step):
        back = dot32(table_ref[pl.ds(plane * step, step), :], second_ref[...])
        back = back.reshape(NEAR, lines, chans).astype(jnp.bfloat16)
        out_refs[0][pl.ds(plane * NEAR, NEAR), 0] = back[:, :keep]
        if len(out_refs) == 2:
            for near in range(NEAR):
                out_refs[1][near ^ (own_ref[0] % NEAR), plane ^ (own_ref[0] // NEAR), 0] = back[
                    near, keep:
                ]


def plane_filter(own, table, w_value, spectrum, pencil, first_band, keep):
    devices, bands, lines, chans = pencil.shape
    cells = devices * lines
    block = lambda count: pl.BlockSpec((devices, 1, count, chans), lambda j, own: (0, j, 0, 0))
    out_specs = [block(keep)]
    out_shape = [jax.ShapeDtypeStruct((devices, bands, keep, chans), jnp.bfloat16)]
    if keep < lines:
        lead, tail = (NEAR, devices // NEAR), (lines - keep, chans)
        out_specs.append(pl.BlockSpec(lead + (1,) + tail, lambda j, own: (0, 0, j, 0, 0)))
        out_shape.append(jax.ShapeDtypeStruct(lead + (bands,) + tail, jnp.bfloat16))
    return pl.pallas_call(
        plane_body,
        name="plane_filter",
        grid_spec=pltpu.PrefetchScalarGridSpec(
            num_scalar_prefetch=1,
            grid=(bands,),
            in_specs=[
                pl.BlockSpec(table.shape, lambda j, own: (0, 0)),
                pl.BlockSpec(w_value.shape, lambda j, own: (0, 0)),
                pl.BlockSpec((1, cells, chans), lambda j, own: (first_band + j, 0, 0)),
                block(lines),
            ],
            out_specs=out_specs,
            scratch_shapes=[pltpu.VMEM((cells, chans), jnp.bfloat16)] * 2,
        ),
        out_shape=out_shape,
        compiler_params=kernel_params(1),
        cost_estimate=pl.CostEstimate(
            flops=2 * bands * cells * chans * (2 * cells + chans),
            bytes_accessed=6 * bands * cells * chans,
            transcendentals=0,
        ),
    )(own, table, w_value, spectrum, pencil)


def finish_body(parts, *refs):
    tables, spectra = refs[:parts], refs[parts : 2 * parts]
    gate_ref, latents_ref, w_out_ref = refs[2 * parts : 2 * parts + 3]
    out_ref, spec_refs = refs[-1 - parts], refs[-parts:]

    @pl.when(pl.program_id(1) == 0)
    def _():
        for source, held in zip(spectra, spec_refs):
            wide = source[...].astype(jnp.float32).reshape(held.shape)
            held[...] = wide.astype(jnp.bfloat16)

    mix = None
    for table_ref, held in zip(tables, spec_refs):
        term = dot32(table_ref[...], held[...], (0, 0))
        mix = term if mix is None else mix + term
    mixed = (mix * gate_ref[...].astype(jnp.float32)).astype(jnp.bfloat16)
    out = latents_ref[...].astype(jnp.float32) + dot32(mixed, w_out_ref[...])
    out_ref[...] = out.astype(jnp.bfloat16)


def finish(tables, spectra, starts, gate, latents, w_out, groups, done=None):
    rows, chans = latents.shape
    group = SUB * WW
    first, count = groups
    pieces = 4
    piece = group // pieces
    by_piece = pl.BlockSpec((piece, chans), lambda g, s: ((first + g) * pieces + s, 0))
    spec_block = lambda spec, start: pl.BlockSpec(
        spec.shape[:2] + (SUB, chans), lambda g, s: (0, 0, first + g - start, 0)
    )
    inputs = [*tables, *spectra, gate, latents, w_out] + ([] if done is None else [done])
    return pl.pallas_call(
        functools.partial(finish_body, len(tables)),
        name="finish",
        grid=(count, pieces),
        in_specs=[
            pl.BlockSpec((table.shape[0], piece), lambda g, s: (0, s)) for table in tables
        ]
        + [spec_block(spec, start) for spec, start in zip(spectra, starts)]
        + [by_piece, by_piece, pl.BlockSpec(w_out.shape, lambda g, s: (0, 0))]
        + ([] if done is None else [pl.BlockSpec(memory_space=pl.ANY)]),
        out_specs=by_piece,
        out_shape=jax.ShapeDtypeStruct((rows, chans), jnp.bfloat16),
        scratch_shapes=[pltpu.VMEM((table.shape[0], chans), jnp.bfloat16) for table in tables],
        input_output_aliases={} if done is None else {len(inputs) - 1: 0},
        compiler_params=kernel_params(2),
        cost_estimate=pl.CostEstimate(
            flops=2 * count * group * chans * (group + chans),
            bytes_accessed=8 * count * group * chans,
            transcendentals=0,
        ),
    )(*inputs)


def tail_body(own_ref, *refs):
    first_table, rest_table, first_ref = refs[:3]
    far = len(refs) - 11
    parts = refs[3 : 3 + far]
    gate_ref, latents_ref, w_out_ref, _, out_ref, first_held, rest_wide, rest_held = refs[3 + far :]

    @pl.when(pl.program_id(0) == 0)
    def _():
        wide = first_ref[...].astype(jnp.float32).reshape(first_held.shape)
        first_held[...] = wide.astype(jnp.bfloat16)
        for offset, part in enumerate(parts):
            plane = offset ^ (own_ref[0] // NEAR)
            for near in range(NEAR):
                source = plane * NEAR + (near ^ (own_ref[0] % NEAR))
                block = part[near].astype(jnp.float32)
                rest_wide[source] = block.reshape(rest_wide.shape[1:])
        rest_held[...] = rest_wide[...].reshape(rest_held.shape).astype(jnp.bfloat16)

    mix = dot32(first_table[...], first_held[...], (0, 0))
    mix = mix + dot32(rest_table[...], rest_held[...], (0, 0))
    mixed = (mix * gate_ref[...].astype(jnp.float32)).astype(jnp.bfloat16)
    out = latents_ref[...].astype(jnp.float32) + dot32(mixed, w_out_ref[...])
    out_ref[...] = out.astype(jnp.bfloat16)


def finish_tail(own, tables, first, parts, gate, latents, w_out, group_at, done):
    rows, chans = latents.shape
    devices = first.shape[0]
    bands = parts[0].shape[1]
    group = SUB * WW
    pieces = 4
    piece = group // pieces
    by_piece = pl.BlockSpec((piece, chans), lambda s, own: (group_at * pieces + s, 0))
    inputs = [own, *tables, first, *parts, gate, latents, w_out, done]
    return pl.pallas_call(
        tail_body,
        name="finish_tail",
        grid_spec=pltpu.PrefetchScalarGridSpec(
            num_scalar_prefetch=1,
            grid=(pieces,),
            in_specs=[
                pl.BlockSpec((table.shape[0], piece), lambda s, own: (0, s)) for table in tables
            ]
            + [pl.BlockSpec(first.shape[:2] + (SUB, chans), lambda s, own: (0, 0, group_at, 0))]
            + [pl.BlockSpec(part.shape, lambda s, own: (0, 0, 0, 0)) for part in parts]
            + [by_piece, by_piece, pl.BlockSpec(w_out.shape, lambda s, own: (0, 0))]
            + [pl.BlockSpec(memory_space=pl.ANY)],
            out_specs=by_piece,
            scratch_shapes=[
                pltpu.VMEM((tables[0].shape[0], chans), jnp.bfloat16),
                pltpu.VMEM((devices, bands * SUB, chans), jnp.float32),
                pltpu.VMEM((tables[1].shape[0], chans), jnp.bfloat16),
            ],
        ),
        out_shape=jax.ShapeDtypeStruct((rows, chans), jnp.bfloat16),
        input_output_aliases={len(inputs) - 1: 0},
        compiler_params=kernel_params(1),
        cost_estimate=pl.CostEstimate(
            flops=2 * group * chans * (group + chans),
            bytes_accessed=8 * group * chans,
            transcendentals=0,
        ),
    )(*inputs)


def relay(tail, devices):
    shift = lambda part, delta: spread_one(part, delta, devices)
    came = [tail[0]] + [shift(tail[near], near) for near in range(1, NEAR)]
    together = [jnp.stack([part[far] for part in came]) for far in range(devices // NEAR)]
    return together[:1] + [shift(part, far * NEAR) for far, part in enumerate(together) if far]


def exchange(tensor):
    return lax.all_to_all(tensor, "sp", split_axis=0, concat_axis=0, tiled=True)


def spread_one(held, delta, devices):
    return lax.ppermute(held, "sp", [(i, i ^ delta) for i in range(devices)])


def spread(held, bits, devices):
    deltas = [0]
    for bit in bits:
        deltas = deltas + [delta ^ bit for delta in deltas]
    blocks = [held]
    for delta in deltas[1:]:
        blocks.append(spread_one(held, delta, devices))
    return blocks, deltas


def gather_blocks(block, stages, devices):
    order = [0]
    held = block[None]
    for bits in stages:
        blocks, deltas = spread(held, bits, devices)
        held = jnp.concatenate(blocks, axis=0)
        order = [slot ^ delta for delta in deltas for slot in order]
    slot_of = jnp.asarray(np.argsort(np.asarray(order)), jnp.int32)
    own = lax.axis_index("sp")
    slots = slot_of[jnp.arange(devices, dtype=jnp.int32) ^ own]
    return jnp.take(held, slots, axis=0)


def gather_stages(devices):
    bits = [1 << at for at in range(devices.bit_length() - 1)]
    return [bits[3:], bits[1:3], bits[:1]]


def chunks_of(band_count):
    return [(0,)] + ([tuple(range(1, band_count))] if band_count > 1 else [])


def local_planes(devices, *args):
    return planes(devices, *args)


def planes(devices, latents, spectrum, w_value, w_gate, w_out, embed_table, prompt_ids, noise_step):
    row_count, chans = latents.shape
    band_count = spectrum.shape[2]
    lines = row_count // WW
    chunks = chunks_of(band_count)
    keep = lines - SUB
    stages = gather_stages(devices)
    each_far = [[bit] for bit in reversed(stages[0])] + stages[1:]
    own = lax.axis_index("sp").astype(jnp.int32)
    tables = [jnp.asarray(width_table(devices, band_count, bands)) for bands in chunks]
    plane = jnp.asarray(plane_table())
    per = w_value.shape[0]

    pencils = []
    for table, bands in zip(tables, chunks):
        part = width_forward(table, latents, devices, len(bands))
        pencils.append(exchange(part))

    both = gather_blocks(jnp.concatenate([w_value, w_gate], axis=0), stages, devices)
    full_value = both[:, :per].reshape(-1, chans)
    full_gate = both[:, per:].reshape(-1, chans)

    taken = jnp.take(embed_table, prompt_ids, axis=1).astype(jnp.float32)
    pooled = jnp.mean(taken, axis=1)
    channel = own * per + jnp.arange(per, dtype=jnp.int32)
    modulation = 1.0 + pooled + step_embedding(noise_step, channel, chans)
    scaled = (w_out.astype(jnp.float32) * modulation[:, None]).astype(jnp.bfloat16)
    full_out = gather_blocks(scaled, each_far, devices).reshape(-1, chans)

    gain = spectrum.transpose(2, 0, 1, 3).reshape(band_count, TT * HH, chans)

    (first,) = plane_filter(own[None], plane, full_value, gain, pencils[0], 0, lines)
    first = exchange(first)
    rest, tail = plane_filter(own[None], plane, full_value, gain, pencils[1], 1, keep)
    rest = exchange(rest)
    tail = relay(tail, devices)

    gate_rows = jnp.dot(latents, full_gate, preferred_element_type=jnp.float32)
    gate = jax.nn.silu(gate_rows).astype(jnp.bfloat16)

    done = finish(tables, [first, rest], [0, 0], gate, latents, full_out, (0, keep // SUB))
    return finish_tail(own[None], tables, first, tail, gate, latents, full_out, keep // SUB, done)


def solution(mesh):
    placed = (
        P(("grp", "sp"), None),
        P(None, None, "sp", "ch"),
        P("sp", "ch"),
        P("sp", "ch"),
        P("sp", None),
        P(("sp", "ch"), None),
        P("grp"),
        P("grp"),
    )
    devices = mesh.shape["sp"]
    lines = TT * HH // devices
    in_planes = (
        mesh.shape["ch"] == 1
        and devices >= 2 * NEAR
        and devices & (devices - 1) == 0
        and WW >= 2 * devices
        and lines >= 2 * SUB
    )
    local = functools.partial(local_planes, devices) if in_planes else local_split_channels
    return jax.shard_map(
        local, mesh=mesh, in_specs=placed, out_specs=P(("grp", "sp", "ch"), None), check_vma=False
    )
```
